32 devices in a mesh: gx: 4 (over z), gy: 4 (over x, core), gz: 2 (over y).
Axes of the slice: x: 2, y: 2, z: 4, core: 2. Of those that a mesh axis runs over, the one named last changes fastest.
Arguments:
- offset: float32 [3, 32, 32, 256], P(None, 'gx', 'gy', 'gz'), may hold values from -0.25 to 0.25
- velocity: float32 [3, 32, 32, 256], P(None, 'gx', 'gy', 'gz'), may hold values from -3 to 3
- spin: float32 [3, 32, 32, 256], P(None, 'gx', 'gy', 'gz'), may hold values from -3 to 3
- radius: float32 [32, 32, 256], P('gx', 'gy', 'gz'), may hold values from 0.62 to 0.82
- history: float32 [6, 3, 32, 32, 256], P(None, None, 'gx', 'gy', 'gz'), may hold values from -0.3 to 0.3
- contacts: int32 [6, 32, 32, 256], P(None, 'gx', 'gy', 'gz'), may hold values from -1 to 8, as said below
- leaving: int32 [4, 4, 2, 64], P('gx', 'gy', 'gz'), may hold values from -1 to 8191, as said below
Outputs:
- new_offset: float32 [3, 32, 32, 256], P(None, 'gx', 'gy', 'gz')
- new_velocity: float32 [3, 32, 32, 256], P(None, 'gx', 'gy', 'gz')
- new_spin: float32 [3, 32, 32, 256], P(None, 'gx', 'gy', 'gz')
- new_history: float32 [6, 3, 32, 32, 256], P(None, None, 'gx', 'gy', 'gz')
- arrivals: float32 [28, 4, 4, 2, 64], P(None, 'gx', 'gy', 'gz')
The draws below stay inside these ranges and needn't reach their ends.
Inputs may be any that keep to these rules, and one draw needn't show every extreme that they name: `contacts`: the live codes of one particle are distinct. `leaving`: each block's live entries are distinct cells with z index 0 or 1 within the block, listed first and followed by -1; at most 64 are live, and some block has 64 live.
All inputs are finite; a program needn't handle non-finite values.
Results may differ from the reference program's by a relative error of at most 0.0003.
Values sent between devices are 32-bit elements; how exact they have to be, the bound alone decides.
A program may use at most 512 MiB of HBM per device.

```python
import jax
import jax.numpy as jnp
import numpy as np
from jax import lax

CX = 8
CY = 8
CZ = 128
K = 6
DIRS = 9
CAP = 64
NX = 32
NY = 32
NZ = 256
N_GX = 4
N_GY = 4
N_GZ = 2


def draw_contacts(key, part):
    alive_key = jax.random.fold_in(key, 11)
    ranking_key = jax.random.fold_in(key, 12)
    height = jnp.arange(NZ, dtype=jnp.int32)
    percent = 95 - 60 * height // NZ
    dice_rolls = jax.random.randint(alive_key, (K, NX, NY, NZ), 0, 100)
    slot_alive = dice_rolls < percent[None, None, None, :]
    scores = jax.random.randint(ranking_key, (DIRS, NX, NY, NZ), 0, 1 << 20) * DIRS + jnp.arange(DIRS, dtype=jnp.int32)[:, None, None, None]
    ranking = jnp.argsort(scores, axis=0, stable=True)[:K].astype(jnp.int32)
    return jnp.where(slot_alive, ranking, -1).astype(jnp.int32)


def draw_leaving(key, part):
    blocks_x = NX // CX
    blocks_y = NY // CY
    blocks_z = NZ // CZ
    choose_key = jax.random.fold_in(key, 21)
    count_key = jax.random.fold_in(key, 22)
    full_key = jax.random.fold_in(key, 23)
    candidates = 2 * CX * CY
    scores = jax.random.randint(choose_key, (blocks_x, blocks_y, blocks_z, candidates), 0, 1 << 20) * candidates + jnp.arange(candidates, dtype=jnp.int32)
    picks = jnp.argsort(scores, axis=-1, stable=True)[..., :CAP].astype(jnp.int32)
    local_x = picks // (2 * CY)
    local_y = picks // 2 % CY
    local_z = picks % 2
    local_cell = (local_x * CY + local_y) * CZ + local_z
    counts = jax.random.randint(count_key, (blocks_x, blocks_y, blocks_z), CAP // 3, CAP + 1)
    chosen_block = jax.random.randint(full_key, (), 0, blocks_x * blocks_y * blocks_z)
    block_number = jnp.arange(blocks_x * blocks_y * blocks_z, dtype=jnp.int32).reshape(blocks_x, blocks_y, blocks_z)
    counts = jnp.where(block_number == chosen_block, CAP, counts)
    slot_number = jnp.arange(CAP, dtype=jnp.int32)
    return jnp.where(slot_number < counts[..., None], local_cell, -1).astype(jnp.int32)


def steps_of(own_key, dims, cuts, low, largest):
    loudness = 1.0
    for axis_at, blocks in cuts:
        draws = jax.random.uniform(jax.random.fold_in(jax.random.fold_in(own_key, 6), axis_at), (blocks,), jnp.float32, low / len(cuts), largest / len(cuts))
        loudness = loudness * jnp.repeat(jnp.exp(draws), dims[axis_at] // blocks).reshape((-1,) + (1,) * (len(dims) - 1 - axis_at))
    return loudness


def bell_draw(own_key, extent, width, bound, shards=(), held_as=jnp.bfloat16):
    loudness = steps_of(own_key, extent, shards, -0.22, 0.18) if shards else 1.0
    entries = jax.random.normal(own_key, extent, jnp.float32) * width * loudness
    return jnp.minimum(jnp.maximum(entries, -bound), bound).astype(held_as)


def setup_inputs(seed: int = 0) -> dict:
    arg_keys = jax.random.split(jax.random.key(seed), 8)
    offset = bell_draw(arg_keys[0], (3, NX, NY, NZ), 0.06, 0.25, ((1, 4), (2, 4), (3, 2)), jnp.float32)
    velocity = bell_draw(arg_keys[1], (3, NX, NY, NZ), 0.5, 3.0, ((1, 4), (2, 4), (3, 2)), jnp.float32)
    spin = bell_draw(arg_keys[2], (3, NX, NY, NZ), 0.5, 3.0, ((1, 4), (2, 4), (3, 2)), jnp.float32)
    radius = jnp.clip(0.62 + 0.19999999 * jax.random.uniform(arg_keys[3], (NX, NY, NZ), jnp.float32) ** steps_of(arg_keys[3], (NX, NY, NZ), ((0, 4), (1, 4), (2, 2)), -0.2, 0.2), 0.62, 0.82)
    history = bell_draw(arg_keys[4], (K, 3, NX, NY, NZ), 0.05, 0.3, ((2, 4), (3, 4), (4, 2)), jnp.float32)
    contacts = draw_contacts(jax.random.fold_in(arg_keys[7], 71), 0)
    leaving = draw_leaving(jax.random.fold_in(arg_keys[7], 71), 0)
    return dict(offset=offset, velocity=velocity, spin=spin, radius=radius, history=history, contacts=contacts, leaving=leaving)


forward_dirs = np.array([[1, 0, 0], [0, 1, 0], [0, 0, 1], [1, 1, 0], [1, -1, 0], [1, 0, 1], [1, 0, -1], [0, 1, 1], [0, 1, -1]], np.int32)
stiff_normal = 10.0
damp_normal = 2.0
stiff_shear = 8.0
damp_shear = 1.5
friction = 0.4
shear_floor = 0.05
time_step = 0.05
gravity = 1.0

def cross_product(first_vec, second_vec):
    return jnp.stack([first_vec[1] * second_vec[2] - first_vec[2] * second_vec[1], first_vec[2] * second_vec[0] - first_vec[0] * second_vec[2], first_vec[0] * second_vec[1] - first_vec[1] * second_vec[0]], 0)

def contact_pair(centers, partner, direction, shear):
    separation = direction + partner[0:3] - centers[0:3]
    distance = jnp.sqrt(lax.optimization_barrier(jnp.sum(separation * separation, 0)))
    normal = separation / distance
    radius_center = centers[9]
    radius_partner = partner[9]
    radius_sum = radius_center + radius_partner
    intersection = jnp.maximum(radius_sum - distance, 0.0)
    contact = jnp.sqrt(radius_center * radius_partner / radius_sum * intersection)
    relative = partner[3:6] - centers[3:6] - cross_product(radius_center * centers[6:9] + radius_partner * partner[6:9], normal)
    approach = lax.optimization_barrier(jnp.sum(relative * normal, 0))
    sliding = relative - approach * normal
    repulsion = jnp.maximum(stiff_normal * contact * intersection - damp_normal * contact * approach, 0.0)
    spring = shear - lax.optimization_barrier(jnp.sum(shear * normal, 0)) * normal + time_step * sliding
    trial_force = stiff_shear * contact * spring + damp_shear * contact * sliding
    magnitude = jnp.sqrt(lax.optimization_barrier(jnp.sum(trial_force * trial_force, 0)))
    factor = jnp.minimum(1.0, friction * repulsion / jnp.maximum(magnitude, shear_floor))
    tangent = factor * trial_force
    pair_force = tangent - repulsion * normal
    twisting = cross_product(normal, tangent)
    return (pair_force, radius_center * twisting, radius_partner * twisting, factor * spring)

def contact_terms(centers, shear, codes, source, base_index, stride_x, stride_y):
    table = jnp.asarray(forward_dirs, dtype=jnp.int32)
    stride_table = table[:, 0] * stride_x + table[:, 1] * stride_y + table[:, 2]
    direction_table = jnp.asarray(forward_dirs.T, dtype=jnp.float32)
    own_terms = jnp.zeros((6, centers.shape[1]), jnp.float32)
    partner_terms = jnp.zeros((6, source.shape[1]), jnp.float32)
    springs = []
    for which_slot in range(codes.shape[0]):
        slot_code = codes[which_slot]
        slot_live = slot_code >= 0
        chosen = jnp.maximum(slot_code, 0)
        selector = chosen[None, :] == jnp.arange(table.shape[0], dtype=jnp.int32)[:, None]
        direction = jnp.dot(direction_table, selector.astype(jnp.float32), precision=lax.Precision.HIGHEST)
        target = base_index + lax.optimization_barrier(jnp.sum(jnp.where(selector, stride_table[:, None], 0), 0)).astype(jnp.int32)
        partner = jnp.take(source, target, axis=1)
        pair_force, torque_center, torque_partner, spring = contact_pair(centers, partner, direction, shear[which_slot])
        own_terms = own_terms + jnp.where(slot_live[None], jnp.concatenate([pair_force, torque_center], 0), 0.0)
        partner_terms = partner_terms.at[:, target].add(jnp.where(slot_live[None], jnp.concatenate([-pair_force, torque_partner], 0), 0.0))
        springs.append(jnp.where(slot_live[None], spring, 0.0))
    return (own_terms, partner_terms, jnp.stack(springs, 0))

def cell_index(count_x, count_y, count_z, margin, span_y, span_z):
    across_x = jnp.arange(count_x, dtype=jnp.int32)[:, None, None] + margin
    across_y = jnp.arange(count_y, dtype=jnp.int32)[None, :, None] + margin
    across_z = jnp.arange(count_z, dtype=jnp.int32)[None, None, :] + margin
    return ((across_x * span_y + across_y) * span_z + across_z).reshape(-1)

def reference(offset, velocity, spin, radius, history, contacts, leaving):
    fields = jnp.concatenate([offset, velocity, spin, radius[None]], 0)
    padded = jnp.pad(fields, ((0, 0), (1, 1), (1, 1), (1, 1)))
    span_y = NY + 2
    span_z = NZ + 2
    base_index = cell_index(NX, NY, NZ, 1, span_y, span_z)
    own_terms, partner_terms, springs = contact_terms(fields.reshape(10, -1), history.reshape(K, 3, -1), contacts.reshape(K, -1), padded.reshape(10, -1), base_index, span_y * span_z, span_z)
    received = partner_terms.reshape(6, NX + 2, span_y, span_z)[:, 1:-1, 1:-1, 1:-1]
    totals = own_terms.reshape(6, NX, NY, NZ) + received
    slot_history = springs.reshape(K, 3, NX, NY, NZ)
    particle_mass = radius ** 3
    downward = jnp.asarray([0.0, 0.0, -gravity], dtype=jnp.float32).reshape(3, 1, 1, 1)
    moved_velocity = velocity + time_step * (totals[0:3] / particle_mass + downward)
    moved_spin = spin + time_step * totals[3:6] / (0.4 * particle_mass * radius * radius)
    moved_offset = offset + time_step * moved_velocity
    coord_x = jnp.broadcast_to(jnp.arange(NX, dtype=jnp.float32)[:, None, None], (NX, NY, NZ))
    coord_y = jnp.broadcast_to(jnp.arange(NY, dtype=jnp.float32)[None, :, None], (NX, NY, NZ))
    coord_z = jnp.broadcast_to(jnp.arange(NZ, dtype=jnp.float32)[None, None, :], (NX, NY, NZ))
    position = jnp.stack([coord_x, coord_y, coord_z], 0) + moved_offset
    leave_live = leaving >= 0
    picked = jnp.maximum(leaving, 0)
    block_x = jnp.arange(N_GX, dtype=jnp.int32)[:, None, None, None]
    block_y = jnp.arange(N_GY, dtype=jnp.int32)[None, :, None, None]
    block_z = jnp.arange(N_GZ, dtype=jnp.int32)[None, None, :, None]
    global_x = block_x * CX + picked // (CY * CZ)
    global_y = block_y * CY + picked // CZ % CY
    global_z = block_z * CZ + picked % CZ
    pieces = [position, moved_velocity, moved_spin, radius[None], slot_history.reshape(3 * K, NX, NY, NZ)]
    outbox = jnp.concatenate([piece[:, global_x, global_y, global_z] for piece in pieces], 0)
    outbox = jnp.where(leave_live[None], outbox, 0.0)
    arrivals = jnp.concatenate([outbox[:, :, :, 1:], jnp.zeros_like(outbox[:, :, :, :1])], 3)
    departed = jnp.zeros((NX, NY, NZ), jnp.float32).at[global_x, global_y, global_z].add(leave_live.astype(jnp.float32))
    staying = 1.0 - departed
    return (moved_offset * staying, moved_velocity * staying, moved_spin * staying, slot_history * staying, arrivals)
```

```python
import functools

import jax
import jax.numpy as jnp
from jax import lax
from jax.experimental import pallas as pl
from jax.experimental.pallas import tpu as pltpu
from jax.sharding import PartitionSpec as P

MESH = pl.DeviceIdType.MESH
AXES = ("gx", "gy", "gz")

forward_dirs = [
    (1, 0, 0),
    (0, 1, 0),
    (0, 0, 1),
    (1, 1, 0),
    (1, -1, 0),
    (1, 0, 1),
    (1, 0, -1),
    (0, 1, 1),
    (0, 1, -1),
]
reach = [
    (1, 0, 0),
    (0, 1, 0),
    (0, -1, 0),
    (0, 0, 1),
    (0, 0, -1),
    (1, 1, 0),
    (1, -1, 0),
    (1, 0, 1),
    (1, 0, -1),
    (0, 1, 1),
    (0, 1, -1),
]
stiff_normal = 10.0
damp_normal = 2.0
stiff_shear = 8.0
damp_shear = 1.5
friction = 0.4
shear_floor = 0.05
time_step = 0.05
gravity = 1.0


def negated(delta):
    return tuple(-step for step in delta)


def dot3(first, second):
    return first[0] * second[0] + first[1] * second[1] + first[2] * second[2]


def cross3(first, second):
    return [
        first[1] * second[2] - first[2] * second[1],
        first[2] * second[0] - first[0] * second[2],
        first[0] * second[1] - first[1] * second[0],
    ]


def kernel(
    sizes,
    offset_in, velocity_in, spin_in, radius_in, history_in, contacts_in, leaving_ref,
    offset_out, velocity_out, spin_out, history_out, arrivals_ref,
    fields, spin, history, contacts, moved, springs_out, stay,
    row_lo, row_hi, halo_yp, halo_ym, face, halo_z,
    sum_c, sum_zp, sum_zm, sum_yp, sum_ym, sum_yzp, sum_yzm,
    rows_p, rows_m, cols, back_x, back_yp, back_ym, back_xy, back_z,
    bottom, picked_rows, outbox, inbox,
    load_sem, store_sem, send_sem, recv_sem, return_send, return_recv, down_sem,
):
    nx = radius_in.shape[0]
    ny, nz = radius_in.shape[1:]
    slots = contacts_in.shape[0]
    me = [lax.axis_index(axis) for axis in AXES]
    f32 = jnp.float32

    def there(delta):
        flag = None
        for place, size, step in zip(me, sizes, delta):
            if step:
                one = (place < size - 1) if step > 0 else (place > 0)
                flag = one if flag is None else jnp.logical_and(flag, one)
        return flag

    def device(delta):
        return tuple(place + step for place, step in zip(me, delta))

    loads = []
    for number, (source, target) in enumerate(
        (
            (offset_in, fields.at[0:3, 0:nx]),
            (velocity_in, fields.at[3:6, 0:nx]),
            (spin_in, spin),
            (radius_in, fields.at[9, 0:nx]),
            (contacts_in, contacts),
            (history_in, history),
        )
    ):
        loads.append(pltpu.make_async_copy(source, target, load_sem.at[number]))
        loads[-1].start()

    barrier = pltpu.get_barrier_semaphore()
    greeted = jnp.int32(0)
    neighbours = []
    for delta in reach:
        for way in (delta, negated(delta)):
            if way not in neighbours:
                neighbours.append(way)
    for way in neighbours:
        flag = there(way)
        greeted = greeted + flag.astype(jnp.int32)

        @pl.when(flag)
        def _(way=way):
            pl.semaphore_signal(barrier, inc=1, device_id=device(way), device_id_type=MESH)

    tile = (ny, nz)
    lane = lax.broadcasted_iota(jnp.int32, tile, 1)
    sub = lax.broadcasted_iota(jnp.int32, tile, 0)
    zero = jnp.zeros(tile, f32)

    def col(value, at):
        return jnp.broadcast_to(value[:, at : at + 1], tile)

    def row(ref, *at):
        return jnp.broadcast_to(ref[at[0], at[1] : at[1] + 1, :], tile)

    def turn_z(value, by):
        return pltpu.roll(value, by % nz, 1)

    def turn_y(value, by):
        return pltpu.roll(value, by % ny, 0)

    leaving = leaving_ref[0, 0]
    wide = jnp.broadcast_to(leaving, (ny, leaving.shape[1]))
    wide_sub = lax.broadcasted_iota(jnp.int32, wide.shape, 0)

    def mark(x, carry):
        gone = zero
        for z in range(2):
            hit = (wide == (x * ny + wide_sub) * nz + z).astype(f32)
            gone = gone + jnp.where(lane == z, jnp.sum(hit, 1, keepdims=True), 0.0)
        stay[x] = 1.0 - gone
        return carry

    lax.fori_loop(0, nx, mark, 0)

    halo_at = [
        fields.at[:, nx],
        halo_yp.at[0:nx],
        halo_ym.at[0:nx],
        halo_z.at[0],
        halo_z.at[1],
        halo_yp.at[nx],
        halo_ym.at[nx],
        halo_z.at[2],
        halo_z.at[3],
        halo_z.at[4],
        halo_z.at[5],
    ]
    back_at = [
        back_x,
        back_yp,
        back_ym,
        back_z.at[0],
        back_z.at[1],
        back_xy.at[0],
        back_xy.at[1],
        back_z.at[2],
        back_z.at[3],
        back_z.at[4],
        back_z.at[5],
    ]
    for delta, halo, back in zip(reach, halo_at, back_at):

        @pl.when(jnp.logical_not(there(delta)))
        def _(halo=halo):
            halo[...] = jnp.zeros(halo.shape, f32)

        @pl.when(jnp.logical_not(there(negated(delta))))
        def _(back=back):
            back[...] = jnp.zeros(back.shape, f32)

    for number in range(6):
        for part in (sum_c, sum_zp, sum_zm, sum_yp, sum_ym):
            part[number, 0] = zero
        for part in (sum_yzp, sum_yzm):
            part[number, nx] = zero

    for number in range(4):
        loads[number].wait()

    def pack(x, faces):
        low, high = faces
        for k in range(3):
            fields[6 + k, x] = spin[k, x] * fields[9, x]
        for c in range(10):
            value = fields[c, x]
            row_lo[x, c : c + 1, :] = value[0:1]
            row_hi[x, c : c + 1, :] = value[ny - 1 : ny]
            here = lane == x * 10 + c
            low = jnp.where(here, col(value, 0), low)
            high = jnp.where(here, col(value, nz - 1), high)
        return low, high

    low, high = lax.fori_loop(0, nx, pack, (zero, zero))
    face[0] = low
    face[1] = high

    pl.semaphore_wait(barrier, greeted)

    sent_from = [
        fields.at[:, 0],
        row_lo,
        row_hi,
        face.at[0],
        face.at[1],
        row_lo.at[0],
        row_hi.at[0],
        face.at[0],
        face.at[1],
        face.at[0],
        face.at[1],
    ]
    order = [5, 6, 7, 8, 9, 10, 0, 1, 2, 3, 4]
    sends = []
    for number, delta in enumerate(reach):
        sends.append(
            pltpu.make_async_remote_copy(
                src_ref=sent_from[number],
                dst_ref=halo_at[number],
                send_sem=send_sem.at[number],
                recv_sem=recv_sem.at[number],
                device_id=device(negated(delta)),
                device_id_type=MESH,
            )
        )
    for number in order:

        @pl.when(there(negated(reach[number])))
        def _(number=number):
            sends[number].start()

    loads[4].wait()
    loads[5].wait()
    for number in range(len(reach)):

        @pl.when(there(reach[number]))
        def _(number=number):
            sends[number].wait_recv()

    span = nx * 10
    col_zp = jnp.where(lane < span, halo_z[0], turn_z(halo_z[2], span))
    col_zm = jnp.where(lane < span, halo_z[1], turn_z(halo_z[3], span))
    col_yzp = jnp.where(sub == ny - 1, turn_y(halo_z[4], -1), turn_y(col_zp, -1))
    col_yzm = jnp.where(sub == ny - 1, turn_y(halo_z[5], -1), turn_y(col_zm, -1))

    def pairs(x, carry):
        own = [fields[c, x] for c in range(10)]
        codes = [contacts[s, x] for s in range(slots)]
        own_sum = [zero] * 6
        springs = []
        for number, (dx, dy, dz) in enumerate(forward_dirs):
            at = x + dx
            other = []
            if dz:
                source = {(0, 1): col_zp, (0, -1): col_zm, (1, 1): col_yzp, (1, -1): col_yzm}[(dy, dz)]
                rim = pltpu.roll(source, nz - at * 10, 1)
            for c in range(10):
                value = fields[c, at]
                if dy > 0:
                    value = jnp.where(sub == ny - 1, row(halo_yp, at, c), turn_y(value, -1))
                elif dy < 0:
                    value = jnp.where(sub == 0, row(halo_ym, at, c), turn_y(value, 1))
                if dz > 0:
                    value = jnp.where(lane == nz - 1, turn_z(rim, nz - 1 - c), turn_z(value, -1))
                elif dz < 0:
                    value = jnp.where(lane == 0, turn_z(rim, -c), turn_z(value, 1))
                other.append(value)
            shear = [zero] * 3
            live = None
            for s in range(slots):
                hit = codes[s] == number
                live = hit if live is None else jnp.logical_or(live, hit)
                for k in range(3):
                    shear[k] = jnp.where(hit, history[s, k, x], shear[k])
            apart = [other[k] - own[k] for k in range(3)]
            for k, step in enumerate((dx, dy, dz)):
                if step:
                    apart[k] = (float(step) + other[k]) - own[k]
            square = dot3(apart, apart)
            inverse = lax.rsqrt(square)
            normal = [part * inverse for part in apart]
            radius_sum = own[9] + other[9]
            inter = jnp.maximum(radius_sum - square * inverse, 0.0)
            contact = jnp.sqrt(own[9] * other[9] / radius_sum * inter)
            turned = cross3([own[6 + k] + other[6 + k] for k in range(3)], normal)
            relative = [other[3 + k] - own[3 + k] - turned[k] for k in range(3)]
            approach = dot3(relative, normal)
            sliding = [relative[k] - approach * normal[k] for k in range(3)]
            repulsion = jnp.maximum(contact * (stiff_normal * inter - damp_normal * approach), 0.0)
            along = dot3(shear, normal)
            spring = [shear[k] - along * normal[k] + time_step * sliding[k] for k in range(3)]
            trial = [contact * (stiff_shear * spring[k] + damp_shear * sliding[k]) for k in range(3)]
            scale = lax.rsqrt(jnp.maximum(dot3(trial, trial), shear_floor * shear_floor))
            factor = jnp.minimum(1.0, friction * repulsion * scale)
            factor = jnp.where(live, factor, 0.0)
            repulsion = jnp.where(live, repulsion, 0.0)
            tangent = [factor * trial[k] for k in range(3)]
            pair = [tangent[k] - repulsion * normal[k] for k in range(3)]
            terms = pair + cross3(normal, tangent)
            springs.append([factor * spring[k] for k in range(3)])
            for c in range(6):
                own_sum[c] = own_sum[c] + terms[c]
            react = [-terms[c] if c < 3 else terms[c] for c in range(6)]
            into = {
                (0, 0): sum_c, (0, 1): sum_zp, (0, -1): sum_zm,
                (1, 0): sum_yp, (-1, 0): sum_ym, (1, 1): sum_yzp, (1, -1): sum_yzm,
            }[(dy, dz)]
            for c in range(6):
                if dx or (dy and dz):
                    into[c, at] = react[c]
                else:
                    into[c, at] += react[c]
        for c in range(6):
            sum_c[c, x] += own_sum[c]
        staying = stay[x]
        packed = jnp.where(lane // 2 == 9, turn_z(own[9], 18), 0.0)
        for s in range(slots):
            for k in range(3):
                value = zero
                for number in range(len(forward_dirs)):
                    value = jnp.where(codes[s] == number, springs[number][k], value)
                springs_out[s, k, x] = value * staying
                place = 10 + 3 * s + k
                packed = jnp.where(lane // 2 == place, turn_z(value, 2 * place), packed)
        bottom[x] = packed
        return carry

    lax.fori_loop(0, nx, pairs, 0)

    history_store = pltpu.make_async_copy(springs_out, history_out, store_sem.at[0])
    history_store.start()

    def split(x, carry):
        face_p, face_m, edge_p, edge_m = carry
        for c in range(6):
            zp, zm = sum_zp[c, x], sum_zm[c, x]
            yp, ym = sum_yp[c, x], sum_ym[c, x]
            yzp, yzm = sum_yzp[c, x], sum_yzm[c, x]
            up = yp + jnp.where(lane == 0, 0.0, turn_z(yzp, 1))
            up = up + jnp.where(lane == nz - 1, 0.0, turn_z(yzm, -1))
            total = sum_c[c, x] + jnp.where(lane == 0, 0.0, turn_z(zp, 1))
            total = total + jnp.where(lane == nz - 1, 0.0, turn_z(zm, -1))
            total = total + jnp.where(sub == 0, 0.0, turn_y(up, 1))
            total = total + jnp.where(sub == ny - 1, 0.0, turn_y(ym, -1))
            sum_c[c, x] = total
            rows_p[x, c : c + 1, :] = up[ny - 1 : ny]
            rows_m[x, c : c + 1, :] = ym[0:1]
            corner_p, corner_m = turn_y(yzp, 1), turn_y(yzm, 1)
            here = lane == x * 8 + c
            face_p = jnp.where(here, col(zp + jnp.where(sub == 0, 0.0, corner_p), nz - 1), face_p)
            face_m = jnp.where(here, col(zm + jnp.where(sub == 0, 0.0, corner_m), 0), face_m)
            edge_p = jnp.where(here, col(corner_p, nz - 1), edge_p)
            edge_m = jnp.where(here, col(corner_m, 0), edge_m)
        return face_p, face_m, edge_p, edge_m

    tiles = lax.fori_loop(0, nx + 1, split, (zero,) * 4)
    for number in range(4):
        cols[number] = tiles[number]

    returned_from = [
        sum_c.at[:, nx],
        rows_p.at[0:nx],
        rows_m.at[0:nx],
        cols.at[0],
        cols.at[1],
        rows_p.at[nx],
        rows_m.at[nx],
        cols.at[0],
        cols.at[1],
        cols.at[2],
        cols.at[3],
    ]
    returns = []
    for number, delta in enumerate(reach):
        returns.append(
            pltpu.make_async_remote_copy(
                src_ref=returned_from[number],
                dst_ref=back_at[number],
                send_sem=return_send.at[number],
                recv_sem=return_recv.at[number],
                device_id=device(delta),
                device_id_type=MESH,
            )
        )
    for number in order:

        @pl.when(there(reach[number]))
        def _(number=number):
            returns[number].start()

    for number, delta in enumerate(reach):

        @pl.when(there(negated(delta)))
        def _(number=number):
            returns[number].wait_recv()

    for c in range(6):
        sum_c[c, 0] += back_x[c]
    back_yp[0] += back_xy[0]
    back_ym[0] += back_xy[1]
    in_zp = back_z[0] + jnp.where(lane < 8, turn_z(back_z[2], -8 * nx), 0.0)
    in_zm = back_z[1] + jnp.where(lane < 8, turn_z(back_z[3], -8 * nx), 0.0)
    in_zp = in_zp + jnp.where(sub == 0, back_z[4], 0.0)
    in_zm = in_zm + jnp.where(sub == 0, back_z[5], 0.0)

    def finish(x, carry):
        staying = stay[x]
        radius = fields[9, x]
        inverse = 1.0 / radius
        cubed = inverse * inverse * inverse
        from_zp = pltpu.roll(in_zp, nz - 8 * x, 1)
        from_zm = pltpu.roll(in_zm, nz - 8 * x, 1)
        totals = []
        for c in range(6):
            total = sum_c[c, x]
            total = total + jnp.where(sub == 0, row(back_yp, x, c), 0.0)
            total = total + jnp.where(sub == ny - 1, row(back_ym, x, c), 0.0)
            total = total + jnp.where(lane == 0, turn_z(from_zp, -c), 0.0)
            total = total + jnp.where(lane == nz - 1, turn_z(from_zm, nz - 1 - c), 0.0)
            totals.append(total)
        coords = (
            (me[0] * nx + x).astype(f32),
            (me[1] * ny + sub).astype(f32),
            (me[2] * nz + lane).astype(f32),
        )
        twisted = (time_step / 0.4) * cubed * inverse
        packed = bottom[x]
        for k in range(3):
            push = totals[k] * cubed
            if k == 2:
                push = push - gravity
            new_velocity = fields[3 + k, x] + time_step * push
            new_spin = spin[k, x] + twisted * totals[3 + k]
            new_offset = fields[k, x] + time_step * new_velocity
            moved[k, x] = new_offset * staying
            moved[3 + k, x] = new_velocity * staying
            moved[6 + k, x] = new_spin * staying
            for place, value in ((k, coords[k] + new_offset), (3 + k, new_velocity), (6 + k, new_spin)):
                packed = jnp.where(lane // 2 == place, turn_z(value, 2 * place), packed)
        bottom[x] = packed
        return carry

    lax.fori_loop(0, nx, finish, 0)

    stores = [history_store]
    for number, target in enumerate((offset_out, velocity_out, spin_out)):
        stores.append(
            pltpu.make_async_copy(moved.at[3 * number : 3 * number + 3], target, store_sem.at[1 + number])
        )
        stores[-1].start()

    cells = bottom[...].reshape(nx * ny, nz)
    capacity = leaving.shape[1]
    cell_number = lax.broadcasted_iota(jnp.int32, (nx * ny, capacity), 0) * nz
    chosen = []
    for z in range(2):
        selector = (cell_number + z == leaving).astype(f32)
        chosen.append(
            lax.dot_general(
                cells, selector, (((0,), (0,)), ((), ())),
                precision=lax.Precision.HIGHEST, preferred_element_type=f32,
            )
        )
    parity = lax.broadcasted_iota(jnp.int32, chosen[0].shape, 0) % 2
    picked_rows[:, 0:capacity] = jnp.where(parity == 0, chosen[0], chosen[1])
    rows = outbox.shape[0]
    outbox[...] = picked_rows[pl.ds(0, rows, stride=2), :] + picked_rows[pl.ds(1, rows, stride=2), :]
    down = pltpu.make_async_remote_copy(
        src_ref=outbox,
        dst_ref=inbox,
        send_sem=down_sem.at[0],
        recv_sem=down_sem.at[1],
        device_id=device((0, 0, -1)),
        device_id_type=MESH,
    )
    has_below, has_above = there((0, 0, -1)), there((0, 0, 1))

    @pl.when(has_below)
    def _():
        down.start()

    for number, delta in enumerate(reach):

        @pl.when(there(negated(delta)))
        def _(number=number):
            sends[number].wait_send()

        @pl.when(there(delta))
        def _(number=number):
            returns[number].wait_send()

    for store in stores:
        store.wait()

    @pl.when(has_below)
    def _():
        down.wait_send()

    @pl.when(has_above)
    def _():
        down.wait_recv()
        arrivals_ref[...] = inbox[:, 0:capacity]

    @pl.when(jnp.logical_not(has_above))
    def _():
        arrivals_ref[...] = jnp.zeros(arrivals_ref.shape, f32)


def on_device(sizes, offset, velocity, spin, radius, history, contacts, leaving):
    nx, ny, nz = radius.shape
    slots = contacts.shape[0]
    rows = 10 + 3 * slots
    capacity = leaving.shape[-1]
    f32 = jnp.float32
    anywhere = pl.BlockSpec(memory_space=pl.ANY)
    near = pl.BlockSpec(memory_space=pltpu.VMEM)
    count = len(reach)
    vmem = lambda *shape: pltpu.VMEM(shape, f32)
    dma = lambda size: pltpu.SemaphoreType.DMA((size,))
    outs = pl.pallas_call(
        functools.partial(kernel, sizes),
        out_shape=(
            jax.ShapeDtypeStruct(offset.shape, f32),
            jax.ShapeDtypeStruct(velocity.shape, f32),
            jax.ShapeDtypeStruct(spin.shape, f32),
            jax.ShapeDtypeStruct(history.shape, f32),
            jax.ShapeDtypeStruct((rows, capacity), f32),
        ),
        in_specs=[anywhere] * 6 + [near],
        out_specs=(anywhere,) * 4 + (near,),
        scratch_shapes=[
            vmem(10, nx + 1, ny, nz),
            vmem(3, nx, ny, nz),
            vmem(slots, 3, nx, ny, nz),
            pltpu.VMEM((slots, nx, ny, nz), jnp.int32),
            vmem(9, nx, ny, nz),
            vmem(slots, 3, nx, ny, nz),
            vmem(nx, ny, nz),
            vmem(nx, 16, nz),
            vmem(nx, 16, nz),
            vmem(nx + 1, 16, nz),
            vmem(nx + 1, 16, nz),
            vmem(2, ny, nz),
            vmem(6, ny, nz),
            *[vmem(6, nx + 1, ny, nz) for part in range(7)],
            vmem(nx + 1, 8, nz),
            vmem(nx + 1, 8, nz),
            vmem(4, ny, nz),
            vmem(6, ny, nz),
            vmem(nx, 8, nz),
            vmem(nx, 8, nz),
            vmem(2, 8, nz),
            vmem(6, ny, nz),
            vmem(nx, ny, nz),
            vmem(nz, nz),
            vmem(rows, nz),
            vmem(rows, nz),
            dma(6),
            dma(4),
            dma(count),
            dma(count),
            dma(count),
            dma(count),
            dma(2),
        ],
        compiler_params=pltpu.CompilerParams(collective_id=0, has_side_effects=True),
    )(offset, velocity, spin, radius, history, contacts, leaving)
    return (*outs[:4], outs[4].reshape(rows, 1, 1, 1, capacity))


def solution(mesh):
    cells = P(None, "gx", "gy", "gz")
    sizes = tuple(mesh.shape[axis] for axis in AXES)
    return jax.shard_map(
        functools.partial(on_device, sizes),
        mesh=mesh,
        in_specs=(
            cells,
            cells,
            cells,
            P("gx", "gy", "gz"),
            P(None, None, "gx", "gy", "gz"),
            cells,
            P("gx", "gy", "gz", None),
        ),
        out_specs=(cells, cells, cells, P(None, None, "gx", "gy", "gz"), P(None, "gx", "gy", "gz", None)),
        check_vma=False,
    )
```

```python
import functools

import jax
import jax.numpy as jnp
from jax import lax
from jax.experimental import pallas as pl
from jax.experimental.pallas import tpu as pltpu
from jax.sharding import PartitionSpec as P

MESH = pl.DeviceIdType.MESH
AXES = ("gx", "gy", "gz")

forward_dirs = [
    (1, 0, 0),
    (0, 1, 0),
    (0, 0, 1),
    (1, 1, 0),
    (1, -1, 0),
    (1, 0, 1),
    (1, 0, -1),
    (0, 1, 1),
    (0, 1, -1),
]
reach = [
    (1, 0, 0),
    (0, 1, 0),
    (0, -1, 0),
    (0, 0, 1),
    (0, 0, -1),
    (1, 1, 0),
    (1, -1, 0),
    (1, 0, 1),
    (1, 0, -1),
    (0, 1, 1),
    (0, 1, -1),
]
stiff_normal = 10.0
damp_normal = 2.0
stiff_shear = 8.0
damp_shear = 1.5
friction = 0.4
shear_floor = 0.05
time_step = 0.05
gravity = 1.0


def negated(delta):
    return tuple(-step for step in delta)


def dot3(first, second):
    return first[0] * second[0] + first[1] * second[1] + first[2] * second[2]


def cross3(first, second):
    return [
        first[1] * second[2] - first[2] * second[1],
        first[2] * second[0] - first[0] * second[2],
        first[0] * second[1] - first[1] * second[0],
    ]


def loop(count, body, carry, unroll):
    if unroll >= count:
        for at in range(count):
            carry = body(at, carry)
        return carry

    def some(step, carry):
        for part in range(unroll):
            carry = body(step * unroll + part, carry)
        return carry

    return lax.fori_loop(0, count // unroll, some, carry)


def kernel(
    sizes,
    offset_in, velocity_in, spin_in, radius_in, history_in, contacts_in, leaving_ref,
    moved, springs_out, arrivals_ref,
    fields, spin, history, contacts, stay,
    row_lo, row_hi, halo_yp, halo_ym, face, halo_z,
    sum_c, sum_zp, sum_zm, sum_yp, sum_ym, sum_yzp, sum_yzm,
    rows_p, rows_m, cols, back_x, back_yp, back_ym, back_xy, back_z,
    bottom, picked_rows, outbox, inbox,
    load_sem, send_sem, recv_sem, return_send, return_recv, down_sem,
):
    nx = radius_in.shape[0]
    ny, nz = radius_in.shape[1:]
    slots = contacts_in.shape[0]
    me = [lax.axis_index(axis) for axis in AXES]
    f32 = jnp.float32

    def there(delta):
        flag = None
        for place, size, step in zip(me, sizes, delta):
            if step:
                one = (place < size - 1) if step > 0 else (place > 0)
                flag = one if flag is None else jnp.logical_and(flag, one)
        return flag

    def device(delta):
        return tuple(place + step for place, step in zip(me, delta))

    loads = []
    for number, (source, target) in enumerate(
        (
            (offset_in, fields.at[0:3, 0:nx]),
            (velocity_in, fields.at[3:6, 0:nx]),
            (spin_in, spin),
            (radius_in, fields.at[9, 0:nx]),
            (contacts_in, contacts),
            (history_in, history),
        )
    ):
        loads.append(pltpu.make_async_copy(source, target, load_sem.at[number]))
        loads[-1].start()

    barrier = pltpu.get_barrier_semaphore()
    greeted = jnp.int32(0)
    neighbours = []
    for delta in reach:
        for way in (delta, negated(delta)):
            if way not in neighbours:
                neighbours.append(way)
    for way in neighbours:
        flag = there(way)
        greeted = greeted + flag.astype(jnp.int32)

        @pl.when(flag)
        def _(way=way):
            pl.semaphore_signal(barrier, inc=1, device_id=device(way), device_id_type=MESH)

    tile = (ny, nz)
    lane = lax.broadcasted_iota(jnp.int32, tile, 1)
    sub = lax.broadcasted_iota(jnp.int32, tile, 0)
    zero = jnp.zeros(tile, f32)

    def col(value, at):
        return jnp.broadcast_to(value[:, at : at + 1], tile)

    def row(ref, *at):
        return jnp.broadcast_to(ref[at[0], at[1] : at[1] + 1, :], tile)

    def turn_z(value, by):
        return pltpu.roll(value, by % nz, 1)

    def turn_x(value, back):
        return pltpu.roll(value, (nz - back) % nz if isinstance(back, int) else nz - back, 1)

    def turn_y(value, by):
        return pltpu.roll(value, by % ny, 0)

    leaving = leaving_ref[0, 0]
    wide = jnp.broadcast_to(leaving, (ny, leaving.shape[1]))
    wide_sub = lax.broadcasted_iota(jnp.int32, wide.shape, 0)

    def mark(x, carry):
        gone = zero
        for z in range(2):
            hit = (wide == (x * ny + wide_sub) * nz + z).astype(f32)
            gone = gone + jnp.where(lane == z, jnp.sum(hit, 1, keepdims=True), 0.0)
        stay[x] = 1.0 - gone
        return carry

    loop(nx, mark, 0, nx)

    halo_at = [
        fields.at[:, nx],
        halo_yp.at[0:nx],
        halo_ym.at[0:nx],
        halo_z.at[0],
        halo_z.at[1],
        halo_yp.at[nx],
        halo_ym.at[nx],
        halo_z.at[2],
        halo_z.at[3],
        halo_z.at[4],
        halo_z.at[5],
    ]
    back_at = [
        back_x,
        back_yp,
        back_ym,
        back_z.at[0],
        back_z.at[1],
        back_xy.at[0],
        back_xy.at[1],
        back_z.at[2],
        back_z.at[3],
        back_z.at[4],
        back_z.at[5],
    ]
    for delta, halo, back in zip(reach, halo_at, back_at):

        @pl.when(jnp.logical_not(there(delta)))
        def _(halo=halo):
            halo[...] = jnp.zeros(halo.shape, f32)

        @pl.when(jnp.logical_not(there(negated(delta))))
        def _(back=back):
            back[...] = jnp.zeros(back.shape, f32)

    for number in range(6):
        for part in (sum_c, sum_zp, sum_zm, sum_yp, sum_ym):
            part[number, 0] = zero
        for part in (sum_yzp, sum_yzm):
            part[number, nx] = zero

    for number in range(4):
        loads[number].wait()

    def pack(x, faces):
        low, high = faces
        for k in range(3):
            fields[6 + k, x] = spin[k, x] * fields[9, x]
        for c in range(10):
            value = fields[c, x]
            row_lo[x, c : c + 1, :] = value[0:1]
            row_hi[x, c : c + 1, :] = value[ny - 1 : ny]
            here = lane == x * 10 + c
            low = jnp.where(here, col(value, 0), low)
            high = jnp.where(here, col(value, nz - 1), high)
        return low, high

    low, high = loop(nx, pack, (zero, zero), nx)
    face[0] = low
    face[1] = high

    pl.semaphore_wait(barrier, greeted)

    sent_from = [
        fields.at[:, 0],
        row_lo,
        row_hi,
        face.at[0],
        face.at[1],
        row_lo.at[0],
        row_hi.at[0],
        face.at[0],
        face.at[1],
        face.at[0],
        face.at[1],
    ]
    order = [5, 6, 7, 8, 9, 10, 0, 1, 2, 3, 4]
    sends = []
    for number, delta in enumerate(reach):
        sends.append(
            pltpu.make_async_remote_copy(
                src_ref=sent_from[number],
                dst_ref=halo_at[number],
                send_sem=send_sem.at[number],
                recv_sem=recv_sem.at[number],
                device_id=device(negated(delta)),
                device_id_type=MESH,
            )
        )
    for number in order:

        @pl.when(there(negated(reach[number])))
        def _(number=number):
            sends[number].start()

    loads[4].wait()
    loads[5].wait()
    for number in range(len(reach)):

        @pl.when(there(reach[number]))
        def _(number=number):
            sends[number].wait_recv()

    span = nx * 10
    col_zp = jnp.where(lane < span, halo_z[0], turn_z(halo_z[2], span))
    col_zm = jnp.where(lane < span, halo_z[1], turn_z(halo_z[3], span))
    col_yzp = jnp.where(sub == ny - 1, turn_y(halo_z[4], -1), turn_y(col_zp, -1))
    col_yzm = jnp.where(sub == ny - 1, turn_y(halo_z[5], -1), turn_y(col_zm, -1))

    def pairs(x, carry):
        own = [fields[c, x] for c in range(10)]
        codes = [contacts[s, x] for s in range(slots)]
        own_sum = [zero] * 6
        springs = []
        for number, (dx, dy, dz) in enumerate(forward_dirs):
            at = x + dx
            other = []
            if dz:
                source = {(0, 1): col_zp, (0, -1): col_zm, (1, 1): col_yzp, (1, -1): col_yzm}[(dy, dz)]
                rim = turn_x(source, at * 10)
            for c in range(10):
                value = fields[c, at]
                if dy > 0:
                    value = jnp.where(sub == ny - 1, row(halo_yp, at, c), turn_y(value, -1))
                elif dy < 0:
                    value = jnp.where(sub == 0, row(halo_ym, at, c), turn_y(value, 1))
                if dz > 0:
                    value = jnp.where(lane == nz - 1, turn_z(rim, nz - 1 - c), turn_z(value, -1))
                elif dz < 0:
                    value = jnp.where(lane == 0, turn_z(rim, -c), turn_z(value, 1))
                other.append(value)
            shear = [zero] * 3
            live = None
            for s in range(slots):
                hit = codes[s] == number
                live = hit if live is None else jnp.logical_or(live, hit)
                for k in range(3):
                    shear[k] = jnp.where(hit, history[s, k, x], shear[k])
            apart = [other[k] - own[k] for k in range(3)]
            for k, step in enumerate((dx, dy, dz)):
                if step:
                    apart[k] = (float(step) + other[k]) - own[k]
            square = dot3(apart, apart)
            inverse = lax.rsqrt(square)
            normal = [part * inverse for part in apart]
            radius_sum = own[9] + other[9]
            inter = jnp.maximum(radius_sum - square * inverse, 0.0)
            contact = jnp.sqrt(own[9] * other[9] / radius_sum * inter)
            turned = cross3([own[6 + k] + other[6 + k] for k in range(3)], normal)
            relative = [other[3 + k] - own[3 + k] - turned[k] for k in range(3)]
            approach = dot3(relative, normal)
            sliding = [relative[k] - approach * normal[k] for k in range(3)]
            repulsion = jnp.maximum(contact * (stiff_normal * inter - damp_normal * approach), 0.0)
            along = dot3(shear, normal)
            spring = [shear[k] - along * normal[k] + time_step * sliding[k] for k in range(3)]
            trial = [contact * (stiff_shear * spring[k] + damp_shear * sliding[k]) for k in range(3)]
            scale = lax.rsqrt(jnp.maximum(dot3(trial, trial), shear_floor * shear_floor))
            factor = jnp.minimum(1.0, friction * repulsion * scale)
            factor = jnp.where(live, factor, 0.0)
            repulsion = jnp.where(live, repulsion, 0.0)
            tangent = [factor * trial[k] for k in range(3)]
            pair = [tangent[k] - repulsion * normal[k] for k in range(3)]
            terms = pair + cross3(normal, tangent)
            springs.append([factor * spring[k] for k in range(3)])
            for c in range(6):
                own_sum[c] = own_sum[c] + terms[c]
            react = [-terms[c] if c < 3 else terms[c] for c in range(6)]
            into = {
                (0, 0): sum_c, (0, 1): sum_zp, (0, -1): sum_zm,
                (1, 0): sum_yp, (-1, 0): sum_ym, (1, 1): sum_yzp, (1, -1): sum_yzm,
            }[(dy, dz)]
            for c in range(6):
                if dx or (dy and dz):
                    into[c, at] = react[c]
                else:
                    into[c, at] += react[c]
        for c in range(6):
            sum_c[c, x] += own_sum[c]
        staying = stay[x]
        packed = jnp.where(lane // 2 == 9, turn_z(own[9], 18), 0.0)
        for s in range(slots):
            for k in range(3):
                value = zero
                for number in range(len(forward_dirs)):
                    value = jnp.where(codes[s] == number, springs[number][k], value)
                springs_out[s, k, x] = value * staying
                place = 10 + 3 * s + k
                packed = jnp.where(lane // 2 == place, turn_z(value, 2 * place), packed)
        bottom[x] = packed
        return carry

    loop(nx, pairs, 0, 1)

    def split(x, carry):
        face_p, face_m, edge_p, edge_m = carry
        for c in range(6):
            zp, zm = sum_zp[c, x], sum_zm[c, x]
            yp, ym = sum_yp[c, x], sum_ym[c, x]
            yzp, yzm = sum_yzp[c, x], sum_yzm[c, x]
            up = yp + jnp.where(lane == 0, 0.0, turn_z(yzp, 1))
            up = up + jnp.where(lane == nz - 1, 0.0, turn_z(yzm, -1))
            total = sum_c[c, x] + jnp.where(lane == 0, 0.0, turn_z(zp, 1))
            total = total + jnp.where(lane == nz - 1, 0.0, turn_z(zm, -1))
            total = total + jnp.where(sub == 0, 0.0, turn_y(up, 1))
            total = total + jnp.where(sub == ny - 1, 0.0, turn_y(ym, -1))
            sum_c[c, x] = total
            rows_p[x, c : c + 1, :] = up[ny - 1 : ny]
            rows_m[x, c : c + 1, :] = ym[0:1]
            corner_p, corner_m = turn_y(yzp, 1), turn_y(yzm, 1)
            here = lane == x * 8 + c
            face_p = jnp.where(here, col(zp + jnp.where(sub == 0, 0.0, corner_p), nz - 1), face_p)
            face_m = jnp.where(here, col(zm + jnp.where(sub == 0, 0.0, corner_m), 0), face_m)
            edge_p = jnp.where(here, col(corner_p, nz - 1), edge_p)
            edge_m = jnp.where(here, col(corner_m, 0), edge_m)
        return face_p, face_m, edge_p, edge_m

    tiles = loop(nx + 1, split, (zero,) * 4, nx + 1)
    for number in range(4):
        cols[number] = tiles[number]

    returned_from = [
        sum_c.at[:, nx],
        rows_p.at[0:nx],
        rows_m.at[0:nx],
        cols.at[0],
        cols.at[1],
        rows_p.at[nx],
        rows_m.at[nx],
        cols.at[0],
        cols.at[1],
        cols.at[2],
        cols.at[3],
    ]
    returns = []
    for number, delta in enumerate(reach):
        returns.append(
            pltpu.make_async_remote_copy(
                src_ref=returned_from[number],
                dst_ref=back_at[number],
                send_sem=return_send.at[number],
                recv_sem=return_recv.at[number],
                device_id=device(delta),
                device_id_type=MESH,
            )
        )
    for number in order:

        @pl.when(there(reach[number]))
        def _(number=number):
            returns[number].start()

    for number, delta in enumerate(reach):

        @pl.when(there(negated(delta)))
        def _(number=number):
            returns[number].wait_recv()

    for c in range(6):
        sum_c[c, 0] += back_x[c]
    back_yp[0] += back_xy[0]
    back_ym[0] += back_xy[1]
    in_zp = back_z[0] + jnp.where(lane < 8, turn_z(back_z[2], -8 * nx), 0.0)
    in_zm = back_z[1] + jnp.where(lane < 8, turn_z(back_z[3], -8 * nx), 0.0)
    in_zp = in_zp + jnp.where(sub == 0, back_z[4], 0.0)
    in_zm = in_zm + jnp.where(sub == 0, back_z[5], 0.0)

    def finish(x, carry):
        staying = stay[x]
        radius = fields[9, x]
        inverse = 1.0 / radius
        cubed = inverse * inverse * inverse
        from_zp = turn_x(in_zp, 8 * x)
        from_zm = turn_x(in_zm, 8 * x)
        totals = []
        for c in range(6):
            total = sum_c[c, x]
            total = total + jnp.where(sub == 0, row(back_yp, x, c), 0.0)
            total = total + jnp.where(sub == ny - 1, row(back_ym, x, c), 0.0)
            total = total + jnp.where(lane == 0, turn_z(from_zp, -c), 0.0)
            total = total + jnp.where(lane == nz - 1, turn_z(from_zm, nz - 1 - c), 0.0)
            totals.append(total)
        coords = (
            (me[0] * nx + x).astype(f32),
            (me[1] * ny + sub).astype(f32),
            (me[2] * nz + lane).astype(f32),
        )
        twisted = (time_step / 0.4) * cubed * inverse
        packed = bottom[x]
        for k in range(3):
            push = totals[k] * cubed
            if k == 2:
                push = push - gravity
            new_velocity = fields[3 + k, x] + time_step * push
            new_spin = spin[k, x] + twisted * totals[3 + k]
            new_offset = fields[k, x] + time_step * new_velocity
            moved[k, x] = new_offset * staying
            moved[3 + k, x] = new_velocity * staying
            moved[6 + k, x] = new_spin * staying
            for place, value in ((k, coords[k] + new_offset), (3 + k, new_velocity), (6 + k, new_spin)):
                packed = jnp.where(lane // 2 == place, turn_z(value, 2 * place), packed)
        bottom[x] = packed
        return carry

    loop(nx, finish, 0, nx)

    cells = bottom[...].reshape(nx * ny, nz)
    capacity = leaving.shape[1]
    cell_number = lax.broadcasted_iota(jnp.int32, (nx * ny, capacity), 0) * nz
    chosen = []
    for z in range(2):
        selector = (cell_number + z == leaving).astype(f32)
        chosen.append(
            lax.dot_general(
                cells, selector, (((0,), (0,)), ((), ())),
                precision=lax.Precision.HIGHEST, preferred_element_type=f32,
            )
        )
    parity = lax.broadcasted_iota(jnp.int32, chosen[0].shape, 0) % 2
    picked_rows[:, 0:capacity] = jnp.where(parity == 0, chosen[0], chosen[1])
    rows = outbox.shape[0]
    outbox[...] = picked_rows[pl.ds(0, rows, stride=2), :] + picked_rows[pl.ds(1, rows, stride=2), :]
    down = pltpu.make_async_remote_copy(
        src_ref=outbox,
        dst_ref=inbox,
        send_sem=down_sem.at[0],
        recv_sem=down_sem.at[1],
        device_id=device((0, 0, -1)),
        device_id_type=MESH,
    )
    has_below, has_above = there((0, 0, -1)), there((0, 0, 1))

    @pl.when(has_below)
    def _():
        down.start()

    for number, delta in enumerate(reach):

        @pl.when(there(negated(delta)))
        def _(number=number):
            sends[number].wait_send()

        @pl.when(there(delta))
        def _(number=number):
            returns[number].wait_send()

    @pl.when(has_below)
    def _():
        down.wait_send()

    @pl.when(has_above)
    def _():
        down.wait_recv()
        arrivals_ref[...] = inbox[:, 0:capacity]

    @pl.when(jnp.logical_not(has_above))
    def _():
        arrivals_ref[...] = jnp.zeros(arrivals_ref.shape, f32)


def emit(moved, springs, arrived, offset_out, velocity_out, spin_out, history_out, arrivals, sem):
    copies = [pltpu.make_async_copy(springs, history_out, sem.at[3])]
    for number, target in enumerate((offset_out, velocity_out, spin_out)):
        source = moved.at[3 * number : 3 * number + 3]
        copies.append(pltpu.make_async_copy(source, target, sem.at[number]))
    for copy in copies:
        copy.start()
    for place in range(arrived.shape[0]):
        arrivals[place, 0, 0] = arrived[place : place + 1, :]
    for copy in copies:
        copy.wait()


def on_device(sizes, offset, velocity, spin, radius, history, contacts, leaving):
    nx, ny, nz = radius.shape
    slots = contacts.shape[0]
    rows = 10 + 3 * slots
    capacity = leaving.shape[-1]
    f32 = jnp.float32
    anywhere = pl.BlockSpec(memory_space=pl.ANY)
    near = pl.BlockSpec(memory_space=pltpu.VMEM)
    count = len(reach)
    vmem = lambda *shape: pltpu.VMEM(shape, f32)
    dma = lambda size: pltpu.SemaphoreType.DMA((size,))
    moved, springs, arrived = pl.pallas_call(
        functools.partial(kernel, sizes),
        out_shape=(
            pltpu.VMEM((9, nx, ny, nz), f32),
            pltpu.VMEM(history.shape, f32),
            pltpu.VMEM((rows, capacity), f32),
        ),
        in_specs=[anywhere] * 6 + [near],
        out_specs=(near,) * 3,
        scratch_shapes=[
            vmem(10, nx + 1, ny, nz),
            vmem(3, nx, ny, nz),
            vmem(slots, 3, nx, ny, nz),
            pltpu.VMEM((slots, nx, ny, nz), jnp.int32),
            vmem(nx, ny, nz),
            vmem(nx, 16, nz),
            vmem(nx, 16, nz),
            vmem(nx + 1, 16, nz),
            vmem(nx + 1, 16, nz),
            vmem(2, ny, nz),
            vmem(6, ny, nz),
            *[vmem(6, nx + 1, ny, nz) for part in range(7)],
            vmem(nx + 1, 8, nz),
            vmem(nx + 1, 8, nz),
            vmem(4, ny, nz),
            vmem(6, ny, nz),
            vmem(nx, 8, nz),
            vmem(nx, 8, nz),
            vmem(2, 8, nz),
            vmem(6, ny, nz),
            vmem(nx, ny, nz),
            vmem(nz, nz),
            vmem(rows, nz),
            vmem(rows, nz),
            dma(6),
            dma(count),
            dma(count),
            dma(count),
            dma(count),
            dma(2),
        ],
        compiler_params=pltpu.CompilerParams(collective_id=0, has_side_effects=True),
    )(offset, velocity, spin, radius, history, contacts, leaving)
    return pl.pallas_call(
        emit,
        out_shape=(
            jax.ShapeDtypeStruct(offset.shape, f32),
            jax.ShapeDtypeStruct(velocity.shape, f32),
            jax.ShapeDtypeStruct(spin.shape, f32),
            jax.ShapeDtypeStruct(history.shape, f32),
            jax.ShapeDtypeStruct((rows, 1, 1, 1, capacity), f32),
        ),
        in_specs=[near] * 3,
        out_specs=(anywhere,) * 4 + (near,),
        scratch_shapes=[dma(4)],
    )(*[pltpu.with_memory_space_constraint(part, pltpu.MemorySpace.VMEM) for part in (moved, springs, arrived)])


def solution(mesh):
    cells = P(None, "gx", "gy", "gz")
    sizes = tuple(mesh.shape[axis] for axis in AXES)
    return jax.shard_map(
        functools.partial(on_device, sizes),
        mesh=mesh,
        in_specs=(
            cells,
            cells,
            cells,
            P("gx", "gy", "gz"),
            P(None, None, "gx", "gy", "gz"),
            cells,
            P("gx", "gy", "gz", None),
        ),
        out_specs=(cells, cells, cells, P(None, None, "gx", "gy", "gz"), P(None, "gx", "gy", "gz", None)),
        check_vma=False,
    )
```

```python
import functools

import jax
import jax.numpy as jnp
from jax import lax
from jax.experimental import pallas as pl
from jax.experimental.pallas import tpu as pltpu
from jax.sharding import PartitionSpec as P

MESH = pl.DeviceIdType.MESH
AXES = ("gx", "gy", "gz")

forward_dirs = [
    (1, 0, 0),
    (0, 1, 0),
    (0, 0, 1),
    (1, 1, 0),
    (1, -1, 0),
    (1, 0, 1),
    (1, 0, -1),
    (0, 1, 1),
    (0, 1, -1),
]
reach = [
    (1, 0, 0),
    (0, 1, 0),
    (0, -1, 0),
    (0, 0, 1),
    (0, 0, -1),
    (1, 1, 0),
    (1, -1, 0),
    (1, 0, 1),
    (1, 0, -1),
    (0, 1, 1),
    (0, 1, -1),
]
stiff_normal = 10.0
damp_normal = 2.0
stiff_shear = 8.0
damp_shear = 1.5
friction = 0.4
shear_floor = 0.05
time_step = 0.05
gravity = 1.0


def negated(delta):
    return tuple(-step for step in delta)


def dot3(first, second):
    return first[0] * second[0] + first[1] * second[1] + first[2] * second[2]


def cross3(first, second):
    return [
        first[1] * second[2] - first[2] * second[1],
        first[2] * second[0] - first[0] * second[2],
        first[0] * second[1] - first[1] * second[0],
    ]


def loop(count, body, carry, unroll):
    if unroll >= count:
        for at in range(count):
            carry = body(at, carry)
        return carry

    def some(step, carry):
        for part in range(unroll):
            carry = body(step * unroll + part, carry)
        return carry

    return lax.fori_loop(0, count // unroll, some, carry)


def kernel(
    sizes,
    offset_in, velocity_in, spin_in, radius_in, history_in, contacts_in, leaving_ref,
    moved, springs_out, arrivals_ref,
    fields, spin, history, contacts, stay, shears, alive, kept,
    row_lo, row_hi, halo_yp, halo_ym, face, halo_z,
    sum_c, sum_zp, sum_zm, sum_yp, sum_ym, sum_yzp, sum_yzm,
    rows_p, rows_m, cols, back_x, back_yp, back_ym, back_xy, back_z,
    bottom, picked_rows, outbox, inbox,
    load_sem, send_sem, recv_sem, return_send, return_recv, down_sem,
):
    nx = radius_in.shape[0]
    ny, nz = radius_in.shape[1:]
    slots = contacts_in.shape[0]
    me = [lax.axis_index(axis) for axis in AXES]
    f32 = jnp.float32

    def there(delta):
        flag = None
        for place, size, step in zip(me, sizes, delta):
            if step:
                one = (place < size - 1) if step > 0 else (place > 0)
                flag = one if flag is None else jnp.logical_and(flag, one)
        return flag

    def device(delta):
        return tuple(place + step for place, step in zip(me, delta))

    loads = []
    for number, (source, target) in enumerate(
        (
            (offset_in, fields.at[0:3, 0:nx]),
            (velocity_in, fields.at[3:6, 0:nx]),
            (spin_in, spin),
            (radius_in, fields.at[9, 0:nx]),
            (contacts_in, contacts),
            (history_in, history),
        )
    ):
        loads.append(pltpu.make_async_copy(source, target, load_sem.at[number]))
        loads[-1].start()

    barrier = pltpu.get_barrier_semaphore()
    greeted = jnp.int32(0)
    neighbours = []
    for delta in reach:
        for way in (delta, negated(delta)):
            if way not in neighbours:
                neighbours.append(way)
    for way in neighbours:
        flag = there(way)
        greeted = greeted + flag.astype(jnp.int32)

        @pl.when(flag)
        def _(way=way):
            pl.semaphore_signal(barrier, inc=1, device_id=device(way), device_id_type=MESH)

    tile = (ny, nz)
    lane = lax.broadcasted_iota(jnp.int32, tile, 1)
    sub = lax.broadcasted_iota(jnp.int32, tile, 0)
    zero = jnp.zeros(tile, f32)

    def col(value, at):
        return jnp.broadcast_to(value[:, at : at + 1], tile)

    def row(ref, *at):
        return jnp.broadcast_to(ref[at[0], at[1] : at[1] + 1, :], tile)

    def turn_z(value, by):
        return pltpu.roll(value, by % nz, 1)

    def turn_x(value, back):
        return pltpu.roll(value, (nz - back) % nz if isinstance(back, int) else nz - back, 1)

    def turn_y(value, by):
        return pltpu.roll(value, by % ny, 0)

    leaving = leaving_ref[0, 0]
    wide = jnp.broadcast_to(leaving, (ny, leaving.shape[1]))
    wide_sub = lax.broadcasted_iota(jnp.int32, wide.shape, 0)

    def mark(x, carry):
        gone = zero
        for z in range(2):
            hit = (wide == (x * ny + wide_sub) * nz + z).astype(f32)
            gone = gone + jnp.where(lane == z, jnp.sum(hit, 1, keepdims=True), 0.0)
        stay[x] = 1.0 - gone
        return carry

    loop(nx, mark, 0, nx)

    halo_at = [
        fields.at[:, nx],
        halo_yp.at[0:nx],
        halo_ym.at[0:nx],
        halo_z.at[0],
        halo_z.at[1],
        halo_yp.at[nx],
        halo_ym.at[nx],
        halo_z.at[2],
        halo_z.at[3],
        halo_z.at[4],
        halo_z.at[5],
    ]
    back_at = [
        back_x,
        back_yp,
        back_ym,
        back_z.at[0],
        back_z.at[1],
        back_xy.at[0],
        back_xy.at[1],
        back_z.at[2],
        back_z.at[3],
        back_z.at[4],
        back_z.at[5],
    ]
    for delta, halo, back in zip(reach, halo_at, back_at):

        @pl.when(jnp.logical_not(there(delta)))
        def _(halo=halo):
            halo[...] = jnp.zeros(halo.shape, f32)

        @pl.when(jnp.logical_not(there(negated(delta))))
        def _(back=back):
            back[...] = jnp.zeros(back.shape, f32)

    for number in range(6):
        for part in (sum_c, sum_zp, sum_zm, sum_yp, sum_ym):
            part[number, 0] = zero
        for part in (sum_yzp, sum_yzm):
            part[number, nx] = zero

    for number in range(4):
        loads[number].wait()

    def pack(x, faces):
        low, high = faces
        for k in range(3):
            fields[6 + k, x] = spin[k, x] * fields[9, x]
        for c in range(10):
            value = fields[c, x]
            row_lo[x, c : c + 1, :] = value[0:1]
            row_hi[x, c : c + 1, :] = value[ny - 1 : ny]
            here = lane == x * 10 + c
            low = jnp.where(here, col(value, 0), low)
            high = jnp.where(here, col(value, nz - 1), high)
        return low, high

    low, high = loop(nx, pack, (zero, zero), nx)
    face[0] = low
    face[1] = high

    pl.semaphore_wait(barrier, greeted)

    sent_from = [
        fields.at[:, 0],
        row_lo,
        row_hi,
        face.at[0],
        face.at[1],
        row_lo.at[0],
        row_hi.at[0],
        face.at[0],
        face.at[1],
        face.at[0],
        face.at[1],
    ]
    order = [5, 6, 7, 8, 9, 10, 0, 1, 2, 3, 4]
    sends = []
    for number, delta in enumerate(reach):
        sends.append(
            pltpu.make_async_remote_copy(
                src_ref=sent_from[number],
                dst_ref=halo_at[number],
                send_sem=send_sem.at[number],
                recv_sem=recv_sem.at[number],
                device_id=device(negated(delta)),
                device_id_type=MESH,
            )
        )
    for number in order:

        @pl.when(there(negated(reach[number])))
        def _(number=number):
            sends[number].start()

    loads[4].wait()
    loads[5].wait()

    def per_direction(x, carry):
        codes = [contacts[s, x] for s in range(slots)]
        for number in range(len(forward_dirs)):
            shear = [zero] * 3
            live = zero
            for s in range(slots):
                hit = codes[s] == number
                live = jnp.where(hit, 1.0, live)
                for k in range(3):
                    shear[k] = jnp.where(hit, history[s, k, x], shear[k])
            alive[x, number] = live
            for k in range(3):
                shears[x, number, k] = shear[k]
        return carry

    loop(nx, per_direction, 0, 1)
    for number in range(len(reach)):

        @pl.when(there(reach[number]))
        def _(number=number):
            sends[number].wait_recv()

    span = nx * 10
    col_zp = jnp.where(lane < span, halo_z[0], turn_z(halo_z[2], span))
    col_zm = jnp.where(lane < span, halo_z[1], turn_z(halo_z[3], span))
    col_yzp = jnp.where(sub == ny - 1, turn_y(halo_z[4], -1), turn_y(col_zp, -1))
    col_yzm = jnp.where(sub == ny - 1, turn_y(halo_z[5], -1), turn_y(col_zm, -1))

    def pairs(x, carry):
        own = [fields[c, x] for c in range(10)]
        own_sum = [zero] * 6
        for number, (dx, dy, dz) in enumerate(forward_dirs):
            at = x + dx
            other = []
            if dz:
                source = {(0, 1): col_zp, (0, -1): col_zm, (1, 1): col_yzp, (1, -1): col_yzm}[(dy, dz)]
                rim = turn_x(source, at * 10)
            for c in range(10):
                value = fields[c, at]
                if dy > 0:
                    value = jnp.where(sub == ny - 1, row(halo_yp, at, c), turn_y(value, -1))
                elif dy < 0:
                    value = jnp.where(sub == 0, row(halo_ym, at, c), turn_y(value, 1))
                if dz > 0:
                    value = jnp.where(lane == nz - 1, turn_z(rim, nz - 1 - c), turn_z(value, -1))
                elif dz < 0:
                    value = jnp.where(lane == 0, turn_z(rim, -c), turn_z(value, 1))
                other.append(value)
            shear = [shears[x, number, k] for k in range(3)]
            live = alive[x, number]
            apart = [other[k] - own[k] for k in range(3)]
            for k, step in enumerate((dx, dy, dz)):
                if step:
                    apart[k] = (float(step) + other[k]) - own[k]
            square = dot3(apart, apart)
            inverse = lax.rsqrt(square)
            normal = [part * inverse for part in apart]
            radius_sum = own[9] + other[9]
            inter = jnp.maximum(radius_sum - square * inverse, 0.0)
            contact = jnp.sqrt(own[9] * other[9] / radius_sum * inter)
            turned = cross3([own[6 + k] + other[6 + k] for k in range(3)], normal)
            relative = [other[3 + k] - own[3 + k] - turned[k] for k in range(3)]
            approach = dot3(relative, normal)
            sliding = [relative[k] - approach * normal[k] for k in range(3)]
            repulsion = jnp.maximum(contact * (stiff_normal * inter - damp_normal * approach), 0.0)
            along = dot3(shear, normal)
            spring = [shear[k] - along * normal[k] + time_step * sliding[k] for k in range(3)]
            trial = [contact * (stiff_shear * spring[k] + damp_shear * sliding[k]) for k in range(3)]
            scale = lax.rsqrt(jnp.maximum(dot3(trial, trial), shear_floor * shear_floor))
            factor = jnp.minimum(1.0, friction * repulsion * scale)
            factor = factor * live
            repulsion = repulsion * live
            tangent = [factor * trial[k] for k in range(3)]
            pair = [tangent[k] - repulsion * normal[k] for k in range(3)]
            terms = pair + cross3(normal, tangent)
            for k in range(3):
                kept[x, number, k] = factor * spring[k]
            for c in range(6):
                own_sum[c] = own_sum[c] + terms[c]
            react = [-terms[c] if c < 3 else terms[c] for c in range(6)]
            into = {
                (0, 0): sum_c, (0, 1): sum_zp, (0, -1): sum_zm,
                (1, 0): sum_yp, (-1, 0): sum_ym, (1, 1): sum_yzp, (1, -1): sum_yzm,
            }[(dy, dz)]
            for c in range(6):
                if dx or (dy and dz):
                    into[c, at] = react[c]
                else:
                    into[c, at] += react[c]
        for c in range(6):
            sum_c[c, x] += own_sum[c]
        return carry

    loop(nx, pairs, 0, 2)

    def per_slot(x, carry):
        codes = [contacts[s, x] for s in range(slots)]
        staying = stay[x]
        packed = jnp.where(lane // 2 == 9, turn_z(fields[9, x], 18), 0.0)
        for s in range(slots):
            for k in range(3):
                value = zero
                for number in range(len(forward_dirs)):
                    value = jnp.where(codes[s] == number, kept[x, number, k], value)
                springs_out[s, k, x] = value * staying
                place = 10 + 3 * s + k
                packed = jnp.where(lane // 2 == place, turn_z(value, 2 * place), packed)
        bottom[x] = packed
        return carry

    def split(x, carry):
        face_p, face_m, edge_p, edge_m = carry
        for c in range(6):
            zp, zm = sum_zp[c, x], sum_zm[c, x]
            yp, ym = sum_yp[c, x], sum_ym[c, x]
            yzp, yzm = sum_yzp[c, x], sum_yzm[c, x]
            up = yp + jnp.where(lane == 0, 0.0, turn_z(yzp, 1))
            up = up + jnp.where(lane == nz - 1, 0.0, turn_z(yzm, -1))
            total = sum_c[c, x] + jnp.where(lane == 0, 0.0, turn_z(zp, 1))
            total = total + jnp.where(lane == nz - 1, 0.0, turn_z(zm, -1))
            total = total + jnp.where(sub == 0, 0.0, turn_y(up, 1))
            total = total + jnp.where(sub == ny - 1, 0.0, turn_y(ym, -1))
            sum_c[c, x] = total
            rows_p[x, c : c + 1, :] = up[ny - 1 : ny]
            rows_m[x, c : c + 1, :] = ym[0:1]
            corner_p, corner_m = turn_y(yzp, 1), turn_y(yzm, 1)
            here = lane == x * 8 + c
            face_p = jnp.where(here, col(zp + jnp.where(sub == 0, 0.0, corner_p), nz - 1), face_p)
            face_m = jnp.where(here, col(zm + jnp.where(sub == 0, 0.0, corner_m), 0), face_m)
            edge_p = jnp.where(here, col(corner_p, nz - 1), edge_p)
            edge_m = jnp.where(here, col(corner_m, 0), edge_m)
        return face_p, face_m, edge_p, edge_m

    tiles = loop(nx + 1, split, (zero,) * 4, nx + 1)
    for number in range(4):
        cols[number] = tiles[number]

    returned_from = [
        sum_c.at[:, nx],
        rows_p.at[0:nx],
        rows_m.at[0:nx],
        cols.at[0],
        cols.at[1],
        rows_p.at[nx],
        rows_m.at[nx],
        cols.at[0],
        cols.at[1],
        cols.at[2],
        cols.at[3],
    ]
    returns = []
    for number, delta in enumerate(reach):
        returns.append(
            pltpu.make_async_remote_copy(
                src_ref=returned_from[number],
                dst_ref=back_at[number],
                send_sem=return_send.at[number],
                recv_sem=return_recv.at[number],
                device_id=device(delta),
                device_id_type=MESH,
            )
        )
    for number in order:

        @pl.when(there(reach[number]))
        def _(number=number):
            returns[number].start()

    loop(nx, per_slot, 0, 1)

    for number, delta in enumerate(reach):

        @pl.when(there(negated(delta)))
        def _(number=number):
            returns[number].wait_recv()

    for c in range(6):
        sum_c[c, 0] += back_x[c]
    back_yp[0] += back_xy[0]
    back_ym[0] += back_xy[1]
    in_zp = back_z[0] + jnp.where(lane < 8, turn_z(back_z[2], -8 * nx), 0.0)
    in_zm = back_z[1] + jnp.where(lane < 8, turn_z(back_z[3], -8 * nx), 0.0)
    in_zp = in_zp + jnp.where(sub == 0, back_z[4], 0.0)
    in_zm = in_zm + jnp.where(sub == 0, back_z[5], 0.0)

    def finish(x, carry):
        staying = stay[x]
        radius = fields[9, x]
        inverse = 1.0 / radius
        cubed = inverse * inverse * inverse
        from_zp = turn_x(in_zp, 8 * x)
        from_zm = turn_x(in_zm, 8 * x)
        totals = []
        for c in range(6):
            total = sum_c[c, x]
            total = total + jnp.where(sub == 0, row(back_yp, x, c), 0.0)
            total = total + jnp.where(sub == ny - 1, row(back_ym, x, c), 0.0)
            total = total + jnp.where(lane == 0, turn_z(from_zp, -c), 0.0)
            total = total + jnp.where(lane == nz - 1, turn_z(from_zm, nz - 1 - c), 0.0)
            totals.append(total)
        coords = (
            (me[0] * nx + x).astype(f32),
            (me[1] * ny + sub).astype(f32),
            (me[2] * nz + lane).astype(f32),
        )
        twisted = (time_step / 0.4) * cubed * inverse
        packed = bottom[x]
        for k in range(3):
            push = totals[k] * cubed
            if k == 2:
                push = push - gravity
            new_velocity = fields[3 + k, x] + time_step * push
            new_spin = spin[k, x] + twisted * totals[3 + k]
            new_offset = fields[k, x] + time_step * new_velocity
            moved[k, x] = new_offset * staying
            moved[3 + k, x] = new_velocity * staying
            moved[6 + k, x] = new_spin * staying
            for place, value in ((k, coords[k] + new_offset), (3 + k, new_velocity), (6 + k, new_spin)):
                packed = jnp.where(lane // 2 == place, turn_z(value, 2 * place), packed)
        bottom[x] = packed
        return carry

    loop(nx, finish, 0, nx)

    cells = bottom[...].reshape(nx * ny, nz)
    capacity = leaving.shape[1]
    cell_number = lax.broadcasted_iota(jnp.int32, (nx * ny, capacity), 0) * nz
    chosen = []
    for z in range(2):
        selector = (cell_number + z == leaving).astype(f32)
        chosen.append(
            lax.dot_general(
                cells, selector, (((0,), (0,)), ((), ())),
                precision=lax.Precision.HIGHEST, preferred_element_type=f32,
            )
        )
    parity = lax.broadcasted_iota(jnp.int32, chosen[0].shape, 0) % 2
    picked_rows[:, 0:capacity] = jnp.where(parity == 0, chosen[0], chosen[1])
    rows = outbox.shape[0]
    outbox[...] = picked_rows[pl.ds(0, rows, stride=2), :] + picked_rows[pl.ds(1, rows, stride=2), :]
    down = pltpu.make_async_remote_copy(
        src_ref=outbox,
        dst_ref=inbox,
        send_sem=down_sem.at[0],
        recv_sem=down_sem.at[1],
        device_id=device((0, 0, -1)),
        device_id_type=MESH,
    )
    has_below, has_above = there((0, 0, -1)), there((0, 0, 1))

    @pl.when(has_below)
    def _():
        down.start()

    for number, delta in enumerate(reach):

        @pl.when(there(negated(delta)))
        def _(number=number):
            sends[number].wait_send()

        @pl.when(there(delta))
        def _(number=number):
            returns[number].wait_send()

    @pl.when(has_below)
    def _():
        down.wait_send()

    @pl.when(has_above)
    def _():
        down.wait_recv()
        arrivals_ref[...] = inbox[:, 0:capacity]

    @pl.when(jnp.logical_not(has_above))
    def _():
        arrivals_ref[...] = jnp.zeros(arrivals_ref.shape, f32)


def emit(moved, springs, arrived, offset_out, velocity_out, spin_out, history_out, arrivals, sem):
    copies = [pltpu.make_async_copy(springs, history_out, sem.at[3])]
    for number, target in enumerate((offset_out, velocity_out, spin_out)):
        source = moved.at[3 * number : 3 * number + 3]
        copies.append(pltpu.make_async_copy(source, target, sem.at[number]))
    for copy in copies:
        copy.start()
    for place in range(arrived.shape[0]):
        arrivals[place, 0, 0] = arrived[place : place + 1, :]
    for copy in copies:
        copy.wait()


def on_device(sizes, offset, velocity, spin, radius, history, contacts, leaving):
    nx, ny, nz = radius.shape
    slots = contacts.shape[0]
    rows = 10 + 3 * slots
    capacity = leaving.shape[-1]
    f32 = jnp.float32
    anywhere = pl.BlockSpec(memory_space=pl.ANY)
    near = pl.BlockSpec(memory_space=pltpu.VMEM)
    count = len(reach)
    vmem = lambda *shape: pltpu.VMEM(shape, f32)
    dma = lambda size: pltpu.SemaphoreType.DMA((size,))
    moved, springs, arrived = pl.pallas_call(
        functools.partial(kernel, sizes),
        out_shape=(
            pltpu.VMEM((9, nx, ny, nz), f32),
            pltpu.VMEM(history.shape, f32),
            pltpu.VMEM((rows, capacity), f32),
        ),
        in_specs=[anywhere] * 6 + [near],
        out_specs=(near,) * 3,
        scratch_shapes=[
            vmem(10, nx + 1, ny, nz),
            vmem(3, nx, ny, nz),
            vmem(slots, 3, nx, ny, nz),
            pltpu.VMEM((slots, nx, ny, nz), jnp.int32),
            vmem(nx, ny, nz),
            vmem(nx, len(forward_dirs), 3, ny, nz),
            vmem(nx, len(forward_dirs), ny, nz),
            vmem(nx, len(forward_dirs), 3, ny, nz),
            vmem(nx, 16, nz),
            vmem(nx, 16, nz),
            vmem(nx + 1, 16, nz),
            vmem(nx + 1, 16, nz),
            vmem(2, ny, nz),
            vmem(6, ny, nz),
            *[vmem(6, nx + 1, ny, nz) for part in range(7)],
            vmem(nx + 1, 8, nz),
            vmem(nx + 1, 8, nz),
            vmem(4, ny, nz),
            vmem(6, ny, nz),
            vmem(nx, 8, nz),
            vmem(nx, 8, nz),
            vmem(2, 8, nz),
            vmem(6, ny, nz),
            vmem(nx, ny, nz),
            vmem(nz, nz),
            vmem(rows, nz),
            vmem(rows, nz),
            dma(6),
            dma(count),
            dma(count),
            dma(count),
            dma(count),
            dma(2),
        ],
        compiler_params=pltpu.CompilerParams(collective_id=0, has_side_effects=True),
    )(offset, velocity, spin, radius, history, contacts, leaving)
    return pl.pallas_call(
        emit,
        out_shape=(
            jax.ShapeDtypeStruct(offset.shape, f32),
            jax.ShapeDtypeStruct(velocity.shape, f32),
            jax.ShapeDtypeStruct(spin.shape, f32),
            jax.ShapeDtypeStruct(history.shape, f32),
            jax.ShapeDtypeStruct((rows, 1, 1, 1, capacity), f32),
        ),
        in_specs=[near] * 3,
        out_specs=(anywhere,) * 4 + (near,),
        scratch_shapes=[dma(4)],
    )(*[pltpu.with_memory_space_constraint(part, pltpu.MemorySpace.VMEM) for part in (moved, springs, arrived)])


def solution(mesh):
    cells = P(None, "gx", "gy", "gz")
    sizes = tuple(mesh.shape[axis] for axis in AXES)
    return jax.shard_map(
        functools.partial(on_device, sizes),
        mesh=mesh,
        in_specs=(
            cells,
            cells,
            cells,
            P("gx", "gy", "gz"),
            P(None, None, "gx", "gy", "gz"),
            cells,
            P("gx", "gy", "gz", None),
        ),
        out_specs=(cells, cells, cells, P(None, None, "gx", "gy", "gz"), P(None, "gx", "gy", "gz", None)),
        check_vma=False,
    )
```
